256 devices in a mesh: groups: 2 (over y), context: 128 (over x, z, core).
Axes of the slice: x: 4, y: 2, z: 16, core: 2. Of those that a mesh axis runs over, the one named last changes fastest.
The devices are a block of a 4x16x16 slice.
Arguments:
- query_proj: bfloat16 [32768, 5120], P(('groups', 'context')), parts along dimension 0, may hold values from -100 to 100
- key_proj: bfloat16 [32768, 1024], P(('groups', 'context')), parts along dimension 0, may hold values from -100 to 100
- values: bfloat16 [32768, 1024], P(('groups', 'context')), parts along dimension 0, may hold values from -6 to 6
- grad_out: bfloat16 [32768, 5120], P(('groups', 'context')), parts along dimension 0, may hold values from -6 to 6
- query_gain: float32 [5120], replicated, may hold values from 0.1 to 1.9
- key_gain: float32 [1024], replicated, may hold values from 0.1 to 1.9
- segments: int32 [32768], P('groups'), parts along dimension 0, may hold values from 0 to 63, never falling along the last dimension, each value on 1 to 512 neighbouring positions
- layout: int32 [512], P('groups'), parts along dimension 0, may hold values from 0 to 255, as said below
Outputs:
- query_grad: bfloat16 [32768, 5120], P(('groups', 'context')), parts along dimension 0
- key_grad: bfloat16 [32768, 1024], P(('groups', 'context')), parts along dimension 0
- value_grad: bfloat16 [32768, 1024], P(('groups', 'context')), parts along dimension 0
- query_gain_grad: float32 [10240], P('groups'), parts along dimension 0
- key_gain_grad: float32 [2048], P('groups'), parts along dimension 0
The draws below stay inside these ranges and needn't reach their ends.
There are 2 independent parts, one for each index of `groups`. The reference program is written for one: setup_inputs(seed, part) draws one part's arguments, and reference() takes and returns one part's arrays. A program takes and returns all parts, laid end to end along the dimension named above; an argument that names none is the same for every part. Nothing has to cross between parts.
Inputs may be any that keep to these rules, and one draw needn't show every extreme that they name: layout is a permutation of the spans; slots are ordered device by device, 2 to a device, and each aligned run of 8 slots holds the spans of one sequence of 512 positions in some order. `segments`: document numbers never fall along the stream; a document has 1 to 512 positions, and one has exactly 512.
All inputs are finite; a program needn't handle non-finite values.
Results may differ from the reference program's by a relative error of at most 0.0086.
Values may be sent and summed in bfloat16 or wider, within the bound.
No kernel may reach another device: no remote copies, remote signals or barrier semaphores. Data moves between devices by JAX's collectives and lax.ppermute only.
A program may use at most 128 MiB of HBM per device.

```python
import math
import jax
import jax.numpy as jnp
import numpy as np
from jax import lax

QUERY_HEADS = 40
KEY_VALUE_HEADS = 8
HEAD_SIZE = 128
SPAN = 64
CPD = 2
SEQ_DEVS = 4
QW = 5120
KW = 1024
TOK_DEV = 128
LENGTH = 512
STREAM_TOKENS = 16384
DOCS = 64
N_CONTEXT = 128


def draw_layout(key, part):
    window = SEQ_DEVS * CPD
    slot_count = STREAM_TOKENS // SPAN
    own_key = jax.random.fold_in(key, 3)
    scores = jax.random.randint(own_key, (slot_count // window, window), 0, 65536) * window + jnp.arange(window, dtype=jnp.int32)[None, :]
    local_order = jnp.argsort(scores, axis=1).astype(jnp.int32)
    starts = jnp.arange(slot_count // window, dtype=jnp.int32)[:, None] * window
    return (local_order + starts).reshape(slot_count).astype(jnp.int32)


def projection_sample(key, salt, width):
    own_key = jax.random.fold_in(key, salt)
    return jnp.clip(jax.random.normal(own_key, (STREAM_TOKENS, width)), -8.0, 8.0).astype(jnp.bfloat16)


def draw_query_proj(key, part):
    return projection_sample(key, 11, QUERY_HEADS * HEAD_SIZE)


def draw_key_proj(key, part):
    return projection_sample(key, 13, KEY_VALUE_HEADS * HEAD_SIZE)


def block_scale(rng, extent, split, low, top_value):
    loudness = 1.0
    for position, shards_of in split:
        steps = jax.random.uniform(jax.random.fold_in(jax.random.fold_in(rng, 6), position), (shards_of,), jnp.float32, low / len(split), top_value / len(split))
        loudness = loudness * jnp.repeat(jnp.exp(steps), extent[position] // shards_of).reshape((-1,) + (1,) * (len(extent) - 1 - position))
    return loudness


def split_up(amount, total, bound, slope):
    loads = [(1 << 20) // math.isqrt(standing ** slope) + 1 for standing in range(2, amount + 1)]
    rest, given = total - bound - (amount - 1), [1] * (amount - 1)
    while rest > 0:
        candidates = [i for i in range(amount - 1) if given[i] < bound]
        whole, budget = sum([loads[i] for i in candidates]), rest
        for i in candidates:
            more = min(bound - given[i], max(1, budget * loads[i] // whole), rest)
            given[i] = given[i] + more
            rest = rest - more
    return np.array([bound] + given)


def uneven_parts(rng, count, total, most, slope):
    if count == 2:
        one = jax.random.randint(rng, (), max(1, total - most), min(most, total - 1) + 1)
        return jnp.stack([one, total - one])
    lengths = jnp.asarray(split_up(count, total, most, slope), jnp.int32)
    twos = (count - 1) // 2
    giver, taker = lengths[1:1 + 2 * twos:2], lengths[2:2 + 2 * twos:2]
    room = jnp.minimum(giver - 1, most - taker)
    moved = jax.random.randint(jax.random.fold_in(rng, 1), (twos,), 0, 1 << 20) % (room + 1)
    lengths = lengths.at[1:1 + 2 * twos:2].set(giver - moved).at[2:2 + 2 * twos:2].set(taker + moved)
    return lengths[jax.random.permutation(jax.random.fold_in(rng, 2), count)]


def noise(key, shape, deviation, most, shards=(), kind=jnp.bfloat16):
    drawn = jax.random.normal(key, shape, jnp.float32) * deviation
    if len(shards) > 0:
        drawn = block_scale(key, shape, shards, -0.22, 0.18) * drawn
    return jnp.clip(drawn, min=-most, max=most).astype(kind)


def setup_inputs(seed: int = 0, part: int = 0) -> dict:
    keys = jax.random.split(jax.random.key(seed), 9)
    part_keys = jax.random.split(jax.random.fold_in(keys[8], part), 9)
    query_proj = draw_query_proj(jax.random.fold_in(jax.random.fold_in(keys[8], part), 71), part)
    key_proj = draw_key_proj(jax.random.fold_in(jax.random.fold_in(keys[8], part), 71), part)
    values = noise(part_keys[2], (STREAM_TOKENS, KW), 1.0, 6.0, ((0, 128),))
    grad_out = noise(part_keys[3], (STREAM_TOKENS, QW), 1.0, 6.0, ((0, 128),))
    query_gain = jnp.clip(1.0 + 0.18 * jax.random.normal(keys[4], (QW,), jnp.float32), 0.1, 1.9)
    key_gain = jnp.clip(1.0 + 0.18 * jax.random.normal(keys[5], (KW,), jnp.float32), 0.1, 1.9)
    segments = jnp.searchsorted(jnp.cumsum(uneven_parts(part_keys[6], DOCS, STREAM_TOKENS, LENGTH, 2)), jnp.arange(STREAM_TOKENS), side="right").astype(jnp.int32)
    layout = draw_layout(jax.random.fold_in(jax.random.fold_in(keys[8], part), 71), part)
    return {"query_proj": query_proj, "key_proj": key_proj, "values": values, "grad_out": grad_out, "query_gain": query_gain, "key_gain": key_gain, "segments": segments, "layout": layout}


NORM_EPS = 1e-06
ROPE_BASE = 500000.0

def rope_angles(positions, head_dim):
    half_dim = head_dim // 2
    inv_freq = jnp.power(ROPE_BASE, -2.0 * jnp.arange(half_dim, dtype=jnp.float32) / head_dim)
    angles = positions.astype(jnp.float32)[:, None] * inv_freq[None, :]
    return (jnp.cos(angles), jnp.sin(angles))

def rotate(inputs, cosine, sine, sign_flip):
    tok_rows = inputs.shape[0]
    half_dim = cosine.shape[1]
    halves = inputs.reshape(tok_rows, inputs.shape[1] // (2 * half_dim), 2, half_dim)
    lower_half = halves[:, :, 0]
    upper_half = halves[:, :, 1]
    cosine_b = cosine[:, None, :]
    sine_b = sine[:, None, :] * sign_flip
    rotated = jnp.stack([lower_half * cosine_b - upper_half * sine_b, upper_half * cosine_b + lower_half * sine_b], axis=2)
    return rotated.reshape(tok_rows, inputs.shape[1])

def norm_forward(inputs, gain_row):
    mean_sq = lax.optimization_barrier(jnp.mean(inputs * inputs, axis=1, keepdims=True))
    factor = lax.rsqrt(mean_sq + NORM_EPS)
    return (inputs * factor * gain_row[None, :], factor)

def norm_backward(inputs, factor, gain_row, upstream):
    weighted = upstream * gain_row[None, :]
    inner_sum = lax.optimization_barrier(jnp.mean(weighted * inputs, axis=1, keepdims=True))
    grad_in = factor * weighted - inputs * factor * factor * factor * inner_sum
    return (grad_in, lax.optimization_barrier(jnp.sum(upstream * inputs * factor, axis=0)))

def head_gradients(queries, key_rows, value_rows, grad_rows, allowed, query_head_group, head_dim):
    tok_rows = queries.shape[0]
    factor = head_dim ** (-0.5)
    query_heads = queries.reshape(tok_rows, query_head_group, head_dim).astype(jnp.float32)
    grad_heads = grad_rows.reshape(tok_rows, query_head_group, head_dim).astype(jnp.float32)
    key_float = key_rows.astype(jnp.float32)
    value_float = value_rows.astype(jnp.float32)
    scores = jnp.einsum('qgd,kd->gqk', query_heads, key_float) * factor
    scores = jnp.where(allowed[None], scores, -jnp.inf)
    row_max = lax.optimization_barrier(jnp.max(scores, axis=2, keepdims=True))
    expo = jnp.exp(scores - row_max)
    attn_probs = expo / lax.optimization_barrier(jnp.sum(expo, axis=2, keepdims=True))
    dprobs = jnp.einsum('qgd,kd->gqk', grad_heads, value_float)
    row_delta = lax.optimization_barrier(jnp.sum(attn_probs * dprobs, axis=2, keepdims=True))
    dscores = (attn_probs * (dprobs - row_delta)).astype(jnp.bfloat16).astype(jnp.float32)
    probs_low = attn_probs.astype(jnp.bfloat16).astype(jnp.float32)
    query_part = jnp.einsum('gqk,kd->qgd', dscores, key_float) * factor
    key_part = jnp.einsum('gqk,qgd->kd', dscores, query_heads) * factor
    value_part = jnp.einsum('gqk,qgd->kd', probs_low, grad_heads)
    return (query_part.reshape(tok_rows, query_head_group * head_dim), key_part, value_part)

def reference(query_proj, key_proj, values, grad_out, query_gain, key_gain, segments, layout):
    query_head_group = QUERY_HEADS // KEY_VALUE_HEADS
    group_width = query_head_group * HEAD_SIZE
    token_index = jnp.arange(STREAM_TOKENS, dtype=jnp.int32)
    positions = (jnp.take(layout, token_index // SPAN) * SPAN + token_index % SPAN).astype(jnp.int32)
    doc_ids = jnp.take(segments, positions)
    cosine, sine = rope_angles(positions % LENGTH, HEAD_SIZE)
    q_inputs = query_proj.astype(jnp.float32)
    k_inputs = key_proj.astype(jnp.float32)
    q_normed, q_factor = norm_forward(q_inputs, query_gain)
    k_normed, k_factor = norm_forward(k_inputs, key_gain)
    q_rope = rotate(q_normed, cosine, sine, 1.0).astype(jnp.bfloat16)
    k_rope = rotate(k_normed, cosine, sine, 1.0).astype(jnp.bfloat16)

    def block_step(carried, device):
        dk_acc, dv_acc = carried
        q_start = (device * TOK_DEV).astype(jnp.int32)
        k_start = (device // SEQ_DEVS * LENGTH).astype(jnp.int32)
        q_block = lax.dynamic_slice_in_dim(q_rope, q_start, TOK_DEV, 0)
        g_block = lax.dynamic_slice_in_dim(grad_out, q_start, TOK_DEV, 0)
        k_block = lax.dynamic_slice_in_dim(k_rope, k_start, LENGTH, 0)
        v_block = lax.dynamic_slice_in_dim(values, k_start, LENGTH, 0)
        pos_query = lax.dynamic_slice_in_dim(positions, q_start, TOK_DEV, 0)
        doc_query = lax.dynamic_slice_in_dim(doc_ids, q_start, TOK_DEV, 0)
        pos_key = lax.dynamic_slice_in_dim(positions, k_start, LENGTH, 0)
        doc_key = lax.dynamic_slice_in_dim(doc_ids, k_start, LENGTH, 0)
        same_seq = pos_key[None, :] // LENGTH == pos_query[:, None] // LENGTH
        allowed = same_seq & (doc_key[None, :] == doc_query[:, None]) & (pos_key[None, :] <= pos_query[:, None])
        query_parts, key_parts, value_parts = ([], [], [])
        for key_value_head in range(KEY_VALUE_HEADS):
            query_part, key_part, value_part = head_gradients(q_block[:, key_value_head * group_width:(key_value_head + 1) * group_width], k_block[:, key_value_head * HEAD_SIZE:(key_value_head + 1) * HEAD_SIZE], v_block[:, key_value_head * HEAD_SIZE:(key_value_head + 1) * HEAD_SIZE], g_block[:, key_value_head * group_width:(key_value_head + 1) * group_width], allowed, query_head_group, HEAD_SIZE)
            query_parts.append(query_part)
            key_parts.append(key_part)
            value_parts.append(value_part)
        key_block_grad = jnp.concatenate(key_parts, axis=1)
        value_block_grad = jnp.concatenate(value_parts, axis=1)
        dk_acc = lax.dynamic_update_slice_in_dim(dk_acc, lax.dynamic_slice_in_dim(dk_acc, k_start, LENGTH, 0) + key_block_grad, k_start, 0)
        dv_acc = lax.dynamic_update_slice_in_dim(dv_acc, lax.dynamic_slice_in_dim(dv_acc, k_start, LENGTH, 0) + value_block_grad, k_start, 0)
        return ((dk_acc, dv_acc), jnp.concatenate(query_parts, axis=1))
    key_zeros = jnp.zeros((STREAM_TOKENS, KEY_VALUE_HEADS * HEAD_SIZE), jnp.float32)
    (dk_rope, dv_sum), dq_blocks = lax.scan(block_step, (key_zeros, key_zeros), jnp.arange(N_CONTEXT, dtype=jnp.int32))
    dq_rope = dq_blocks.reshape(STREAM_TOKENS, QUERY_HEADS * HEAD_SIZE)
    dq_normed = rotate(dq_rope, cosine, sine, -1.0)
    dk_normed = rotate(dk_rope, cosine, sine, -1.0)
    query_grad, query_gain_grad = norm_backward(q_inputs, q_factor, query_gain, dq_normed)
    key_grad, key_gain_grad = norm_backward(k_inputs, k_factor, key_gain, dk_normed)
    return (query_grad.astype(jnp.bfloat16), key_grad.astype(jnp.bfloat16), dv_sum.astype(jnp.bfloat16), query_gain_grad, key_gain_grad)
```

```python
import functools

import jax
import jax.numpy as jnp
from jax import lax
from jax.experimental import pallas as pl
from jax.experimental.pallas import tpu as pltpu
from jax.sharding import Mesh
from jax.sharding import PartitionSpec as P

HEADS = 40
KV = 8
REP = HEADS // KV
D = 128
HALF = D // 2
SPAN = 64
SPANS = 8
LENGTH = 512
TOK = 128
QW = HEADS * D
KW = KV * D
GW = REP * D
EPS = 1e-06
ROPE_BASE = 500000.0
SCALE = D ** (-0.5)
LOG2E = 1.4426950408889634
X, Z, C = "context_0", "context_1", "context_2"
CONTEXT = (X, Z, C)
GROUPS_CONTEXT = ("groups",) + CONTEXT
F32 = jnp.float32
BF16 = jnp.bfloat16
NT = (((1,), (1,)), ((), ()))


def partner(block, axis, bits):
    count = lax.axis_size(axis)
    return lax.ppermute(block, axis, [(i, i ^ bits) for i in range(count)])


def roll_half(x):
    return pltpu.roll(x, HALF, 1)


def query_kernel(q_ref, gain_ref, cos_ref, sin_ref, rope_ref, factor_ref):
    acc = jnp.zeros((TOK, D), F32)
    for h in range(HEADS):
        x = q_ref[:, h * D : (h + 1) * D].astype(F32)
        acc = acc + x * x
    factor = lax.rsqrt(jnp.sum(acc, axis=1, keepdims=True) * (1.0 / QW) + EPS)
    factor_ref[...] = jnp.broadcast_to(factor, (TOK, D))
    fb = factor_ref[...]
    cos = cos_ref[...]
    sin = sin_ref[...]
    for h in range(HEADS):
        cols = slice(h * D, (h + 1) * D)
        x = q_ref[:, cols].astype(F32) * fb * gain_ref[:, cols]
        rope_ref[:, cols] = (x * cos + roll_half(x) * sin).astype(BF16)


def key_kernel(k0, k1, k2, k3, gain_ref, cos_ref, sin_ref, rope_ref, trans_ref, hat_ref):
    for b, k_ref in enumerate((k0, k1, k2, k3)):
        rows = slice(b * TOK, (b + 1) * TOK)
        acc = jnp.zeros((TOK, D), F32)
        for h in range(KV):
            x = k_ref[:, h * D : (h + 1) * D].astype(F32)
            acc = acc + x * x
        factor = lax.rsqrt(jnp.sum(acc, axis=1, keepdims=True) * (1.0 / KW) + EPS)
        cos = cos_ref[rows, :]
        sin = sin_ref[rows, :]
        for h in range(KV):
            cols = slice(h * D, (h + 1) * D)
            hat = k_ref[:, cols].astype(F32) * factor
            hat_ref[rows, cols] = hat
            x = hat * gain_ref[:, cols]
            out = x * cos + roll_half(x) * sin
            rope_ref[rows, cols] = out.astype(BF16)
            trans_ref[cols, rows] = out.T.astype(BF16)


def attention_kernel(
    qr_ref,
    g_ref,
    q_ref,
    kr_ref,
    kt_ref,
    hat_ref,
    v0,
    v1,
    v2,
    v3,
    bias_ref,
    cos_ref,
    sin_ref,
    cost_ref,
    sint_ref,
    factor_ref,
    qgain_ref,
    own_ref,
    far_ref,
    send_near_ref,
    send_diag_ref,
    gain_ref,
    qgrad_ref,
    v_scr,
    p_scr,
    ds_scr,
    q5_scr,
    g5_scr,
    w_scr,
    qs_scr,
    inner_scr,
):
    h = pl.program_id(0)

    @pl.when(h == 0)
    def _():
        inner_scr[...] = jnp.zeros_like(inner_scr)

    for b, ref in enumerate((v0, v1, v2, v3)):
        v_scr[b * TOK : (b + 1) * TOK, :] = ref[...]
    for i in range(REP):
        q5_scr[i * TOK : (i + 1) * TOK, :] = qr_ref[:, i * D : (i + 1) * D]
        g5_scr[i * TOK : (i + 1) * TOK, :] = g_ref[:, i * D : (i + 1) * D]
    keys = kr_ref[...]
    vals = v_scr[...]
    for i in range(REP):
        rows = slice(i * TOK, (i + 1) * TOK)
        s = lax.dot_general(keys, q5_scr[rows, :], NT, preferred_element_type=F32)
        s = s + bias_ref[...]
        m = jnp.max(s, axis=0, keepdims=True)
        e = jnp.exp2((s - m) * (SCALE * LOG2E))
        p = e * (1.0 / jnp.sum(e, axis=0, keepdims=True))
        dp = lax.dot_general(vals, g5_scr[rows, :], NT, preferred_element_type=F32)
        delta = jnp.sum(p * dp, axis=0, keepdims=True)
        p_scr[:, rows] = p.astype(BF16)
        ds_scr[:, rows] = (p * (dp - delta)).astype(BF16)
    dv = jnp.dot(p_scr[...], g5_scr[...], preferred_element_type=F32)
    dk = jnp.dot(ds_scr[...], q5_scr[...], preferred_element_type=F32) * SCALE
    own_ref[0] = dk[0:TOK]
    own_ref[1] = dv[0:TOK]
    send_near_ref[0] = dk[TOK : 2 * TOK].astype(BF16)
    send_near_ref[1] = dv[TOK : 2 * TOK].astype(BF16)
    far_ref[0] = dk[2 * TOK : 3 * TOK]
    far_ref[1] = dv[2 * TOK : 3 * TOK]
    send_diag_ref[0] = dk[3 * TOK :].astype(BF16)
    send_diag_ref[1] = dv[3 * TOK :].astype(BF16)
    dkn = dk * cos_ref[...] - roll_half(dk) * sin_ref[...]
    gain_ref[0, REP : REP + 1, :] = jnp.sum(dkn * hat_ref[...], axis=0, keepdims=True)

    dqt = jnp.dot(kt_ref[...], ds_scr[...], preferred_element_type=F32)
    cost = cost_ref[...]
    sint = sint_ref[...]
    acc = inner_scr[...]
    factor = factor_ref[...]
    for i in range(REP):
        cols = slice(i * D, (i + 1) * D)
        da = dqt[0:HALF, cols]
        db = dqt[HALF:, cols]
        dqn = jnp.concatenate([da * cost + db * sint, db * cost - da * sint], axis=0).T
        q = q_ref[:, cols].astype(F32)
        gain_ref[0, i : i + 1, :] = jnp.sum(dqn * q * factor, axis=0, keepdims=True)
        w = dqn * qgain_ref[:, cols]
        acc = acc + w * q
        w_scr[h, :, cols] = w
        qs_scr[h, :, cols] = q_ref[:, cols]
    inner_scr[...] = acc
    gain_ref[0, REP + 1 :, :] = jnp.zeros((8 - REP - 1, D), F32)

    @pl.when(h == KV - 1)
    def _():
        inner = jnp.sum(inner_scr[...], axis=1, keepdims=True) * (1.0 / QW)
        coef = factor * factor * factor * inner
        for j in range(KV):
            for i in range(REP):
                cols = slice(i * D, (i + 1) * D)
                out = factor * w_scr[j, :, cols] - qs_scr[j, :, cols].astype(F32) * coef
                qgrad_ref[:, j * GW + i * D : j * GW + (i + 1) * D] = out.astype(BF16)


def finish_kernel(own_ref, near_ref, far_ref, k_ref, gain_ref, cos_ref, sin_ref, kgrad_ref, vgrad_ref):
    acc = jnp.zeros((TOK, D), F32)
    for h in range(KV):
        x = k_ref[:, h * D : (h + 1) * D].astype(F32)
        acc = acc + x * x
    factor = lax.rsqrt(jnp.sum(acc, axis=1, keepdims=True) * (1.0 / KW) + EPS)
    cos = cos_ref[...]
    sin = sin_ref[...]
    acc = jnp.zeros((TOK, D), F32)
    parts = []
    for h in range(KV):
        cols = slice(h * D, (h + 1) * D)
        dv = own_ref[1, :, cols] + near_ref[1, :, cols].astype(F32) + far_ref[1, :, cols].astype(F32)
        vgrad_ref[:, cols] = dv.astype(BF16)
        dk = own_ref[0, :, cols] + near_ref[0, :, cols].astype(F32) + far_ref[0, :, cols].astype(F32)
        w = (dk * cos - roll_half(dk) * sin) * gain_ref[:, cols]
        acc = acc + w * k_ref[:, cols].astype(F32)
        parts.append(w)
    inner = jnp.sum(acc, axis=1, keepdims=True) * (1.0 / KW)
    coef = factor * factor * factor * inner
    for h in range(KV):
        cols = slice(h * D, (h + 1) * D)
        out = factor * parts[h] - k_ref[:, cols].astype(F32) * coef
        kgrad_ref[:, cols] = out.astype(BF16)


def shape(dims, dtype=F32):
    return jax.ShapeDtypeStruct(dims, dtype)


def whole(count):
    return [pl.BlockSpec(memory_space=pltpu.VMEM)] * count


PARAMS = dict(vmem_limit_bytes=32 * 1024 * 1024)


def pick(table, index):
    chosen = index[:, None] == jnp.arange(table.shape[0], dtype=jnp.int32)[None, :]
    chosen = chosen.reshape(chosen.shape + (1,) * (table.ndim - 1))
    return jnp.sum(jnp.where(chosen, table[None], 0), axis=1)


def sum_gains(part):
    part = part + partner(part, C, 1)
    part = part + partner(part, X, 1) + partner(part, X, 2) + partner(part, X, 3)
    part = part + partner(part, Z, 1) + partner(part, Z, 2) + partner(part, Z, 3)
    return part + partner(part, Z, 4) + partner(part, Z, 8) + partner(part, Z, 12)


def body(query_proj, key_proj, values, grad_out, query_gain, key_gain, segments, layout):
    my_index = lax.axis_index(CONTEXT)
    rank = my_index % 4
    sequence = my_index // 4

    far_k = partner(key_proj, Z, 1)
    near_k = partner(key_proj, C, 1)
    far_v = partner(values, Z, 1)
    near_v = partner(values, C, 1)
    diag_k = partner(far_k, C, 1)
    diag_v = partner(far_v, C, 1)

    slots = lax.dynamic_slice(layout, (sequence * SPANS,), (SPANS,)) % SPANS
    segs = lax.dynamic_slice(segments, (sequence * LENGTH,), (LENGTH,)).reshape(SPANS, SPAN)
    j = jnp.arange(SPANS, dtype=jnp.int32)
    order = pick(slots, jnp.bitwise_xor(rank, j // 2) * 2 + j % 2)
    doc = pick(segs, order).reshape(LENGTH)
    pos = (order[:, None] * SPAN + jnp.arange(SPAN, dtype=jnp.int32)[None, :]).reshape(LENGTH)
    allowed = (doc[:, None] == doc[None, :TOK]) & (pos[:, None] <= pos[None, :TOK])
    bias = jnp.where(allowed, 0.0, -jnp.inf).astype(F32)

    lane = jnp.arange(D, dtype=jnp.int32)
    inv_freq = jnp.power(ROPE_BASE, -2.0 * (lane % HALF).astype(F32) / D)
    angles = pos.astype(F32)[:, None] * inv_freq[None, :]
    cos = jnp.cos(angles)
    sin = jnp.sin(angles) * jnp.where(lane < HALF, -1.0, 1.0)[None, :]
    cost = cos[:TOK, :HALF].T * SCALE
    sint = sin[:TOK, HALF:].T * SCALE
    qgain = query_gain.reshape(1, QW)
    kgain = key_gain.reshape(1, KW)

    q_rope, factor = pl.pallas_call(
        query_kernel,
        out_shape=(shape((TOK, QW), BF16), shape((TOK, D))),
        in_specs=whole(4),
        out_specs=tuple(whole(2)),
        compiler_params=pltpu.CompilerParams(**PARAMS),
        name="query_prep",
    )(query_proj, qgain, cos[:TOK], sin[:TOK])

    k_rope, k_trans, k_hat = pl.pallas_call(
        key_kernel,
        out_shape=(shape((LENGTH, KW), BF16), shape((KW, LENGTH), BF16), shape((LENGTH, KW))),
        in_specs=whole(7),
        out_specs=tuple(whole(3)),
        compiler_params=pltpu.CompilerParams(**PARAMS),
        name="key_prep",
    )(key_proj, near_k, far_k, diag_k, kgain, cos, sin)

    def cols(rows, width):
        return pl.BlockSpec((rows, width), lambda h: (0, h))

    def full(rows, width):
        return pl.BlockSpec((rows, width), lambda h: (0, 0))

    pair = pl.BlockSpec((2, TOK, D), lambda h: (0, 0, h))
    own, far, send_near, send_diag, gains, query_grad = pl.pallas_call(
        attention_kernel,
        grid=(KV,),
        out_shape=(
            shape((2, TOK, KW)),
            shape((2, TOK, KW)),
            shape((2, TOK, KW), BF16),
            shape((2, TOK, KW), BF16),
            shape((KV, 8, D)),
            shape((TOK, QW), BF16),
        ),
        in_specs=[
            cols(TOK, GW),
            cols(TOK, GW),
            cols(TOK, GW),
            cols(LENGTH, D),
            pl.BlockSpec((D, LENGTH), lambda h: (h, 0)),
            cols(LENGTH, D),
            cols(TOK, D),
            cols(TOK, D),
            cols(TOK, D),
            cols(TOK, D),
            full(LENGTH, TOK),
            full(LENGTH, D),
            full(LENGTH, D),
            full(HALF, TOK),
            full(HALF, TOK),
            full(TOK, D),
            cols(1, GW),
        ],
        out_specs=(
            pair,
            pair,
            pair,
            pair,
            pl.BlockSpec((1, 8, D), lambda h: (h, 0, 0)),
            full(TOK, QW),
        ),
        scratch_shapes=[
            pltpu.VMEM((LENGTH, D), BF16),
            pltpu.VMEM((LENGTH, GW), BF16),
            pltpu.VMEM((LENGTH, GW), BF16),
            pltpu.VMEM((GW, D), BF16),
            pltpu.VMEM((GW, D), BF16),
            pltpu.VMEM((KV, TOK, GW), F32),
            pltpu.VMEM((KV, TOK, GW), BF16),
            pltpu.VMEM((TOK, D), F32),
        ],
        compiler_params=pltpu.CompilerParams(**PARAMS),
        name="attention",
    )(
        q_rope,
        grad_out,
        query_proj,
        k_rope,
        k_trans,
        k_hat,
        values,
        near_v,
        far_v,
        diag_v,
        bias,
        cos,
        sin,
        cost,
        sint,
        factor,
        qgain,
    )

    back_diag = partner(send_diag, C, 1)
    send_far = (far + back_diag.astype(F32)).astype(BF16)
    back_far = partner(send_far, Z, 1)
    back_near = partner(send_near, C, 1)
    gains = sum_gains(gains)
    key_grad, value_grad = pl.pallas_call(
        finish_kernel,
        out_shape=(shape((TOK, KW), BF16), shape((TOK, KW), BF16)),
        in_specs=whole(7),
        out_specs=tuple(whole(2)),
        compiler_params=pltpu.CompilerParams(**PARAMS),
        name="key_finish",
    )(own, back_near, back_far, key_proj, kgain, cos[:TOK], sin[:TOK])
    return (
        query_grad,
        key_grad,
        value_grad,
        gains[:, :REP].reshape(QW),
        gains[:, REP].reshape(KW),
    )


def solution(mesh):
    split = Mesh(
        mesh.devices.reshape(mesh.shape["groups"], 4, 16, 2),
        ("groups",) + CONTEXT,
    )
    rows = P(GROUPS_CONTEXT, None)
    placed = (rows, rows, rows, rows, P(), P(), P("groups"), P("groups"))
    return jax.shard_map(
        body,
        mesh=split,
        in_specs=placed,
        out_specs=(rows, rows, rows, P("groups"), P("groups")),
        check_vma=False,
    )
```
